32 devices in a mesh: section: 4 (over y, core), tensor: 4 (over z), dp: 2 (over x).
Axes of the slice: x: 2, y: 2, z: 4, core: 2. Of those that a mesh axis runs over, the one named last changes fastest.
Arguments:
- section_up: bfloat16 [4, 4096, 7168], P('section', 'dp', 'tensor'), may hold values from -0.09375 to 0.09375
- section_down: bfloat16 [4, 4096, 7168], P('section', 'dp', 'tensor'), may hold values from -0.0625 to 0.0625
- backup_up: bfloat16 [2, 4, 4, 128, 7168], P('dp', 'section', 'tensor'), may hold values from -0.09375 to 0.09375
- backup_down: bfloat16 [2, 4, 4, 128, 7168], P('dp', 'section', 'tensor'), may hold values from -0.0625 to 0.0625
- norm_gain: float32 [4, 4096], P('section'), may hold values from 0.25 to 1.75
- micro_batches: bfloat16 [4, 64, 4096], P(None, 'dp', 'tensor'), may hold values from -24 to 24
- failed_section: int32 [1], replicated, may hold values from 0 to 262143
- live_batches: int32 [1], replicated, may hold values from 0 to 196607
Outputs:
- finals: bfloat16 [4, 64, 4096], P('section', 'dp', 'tensor')
The draws below stay inside these ranges and needn't reach their ends.
Inputs may be any that keep to these rules, and one draw needn't show every extreme that they name: failed_section modulo the number of sections names the failed section. micro-batches 0 to 4 // 2 + (live_batches modulo (4 - 4 // 2 + 1)) - 1 run.
All inputs are finite; a program needn't handle non-finite values.
Results may differ from the reference program's by a relative error of at most 0.03.
Values may be sent and summed in bfloat16 or wider, within the bound.
A program may use at most 192 MiB of HBM per device.

```python
import math
import jax
import jax.numpy as jnp
from jax import lax

D = 4096
FF = 7168
MB = 4
TOKENS_MB = 64
ROWS_PIECE = 128
N_SECTION = 4
N_TENSOR = 4
N_DP = 2


def draw_micro_batches(key, part):
    first, second, third = jax.random.split(key, 3)
    shape = (MB, TOKENS_MB, D)
    row_scale = jnp.exp(jax.random.uniform(second, (MB, TOKENS_MB, 1), jnp.float32, math.log(0.3), math.log(3.0)))
    column_scale = jnp.exp(jax.random.uniform(third, (1, 1, D), jnp.float32, math.log(0.3), math.log(3.0)))
    values = jax.random.normal(first, shape, jnp.float32) * row_scale * column_scale
    return jnp.clip(values, -24.0, 24.0).astype(jnp.bfloat16)


def shard_levels(rng, extent, pieces, smallest, top_value):
    factor_of = 1.0
    for dim, shards_of in pieces:
        draws = jax.random.uniform(jax.random.fold_in(jax.random.fold_in(rng, 6), dim), (shards_of,), jnp.float32, smallest / len(pieces), top_value / len(pieces))
        factor_of = factor_of * jnp.repeat(jnp.exp(draws), extent[dim] // shards_of).reshape((-1,) + (1,) * (len(extent) - 1 - dim))
    return factor_of


def gaussian(key, shape, deviation, limit, shards=(), kind=jnp.bfloat16):
    entries = jax.random.normal(key, shape, jnp.float32) * deviation
    if len(shards) > 0:
        entries = shard_levels(key, shape, shards, -0.22, 0.18) * entries
    return jnp.clip(entries, min=-limit, max=limit).astype(kind)


def setup_inputs(seed: int = 0) -> dict:
    key_of = jax.random.split(jax.random.key(seed), 9)
    section_up = gaussian(key_of[0], (N_SECTION, D, FF), D ** -0.5, 0.09375, ((0, 4), (1, 2), (2, 4)))
    section_down = gaussian(key_of[1], (N_SECTION, D, FF), FF ** -0.5, 0.0625, ((0, 4), (1, 2), (2, 4)))
    backup_up = gaussian(key_of[2], (N_DP, N_SECTION, N_TENSOR, ROWS_PIECE, FF), D ** -0.5, 0.09375, ((0, 2), (1, 4), (2, 4)))
    backup_down = gaussian(key_of[3], (N_DP, N_SECTION, N_TENSOR, ROWS_PIECE, FF), FF ** -0.5, 0.0625, ((0, 2), (1, 4), (2, 4)))
    norm_gain = jnp.clip(1.0 + 0.15 * jax.random.normal(key_of[4], (N_SECTION, D), jnp.float32), 0.25, 1.75)
    micro_batches = draw_micro_batches(jax.random.fold_in(key_of[8], 71), 0)
    failed_section = jax.random.randint(key_of[6], (1,), 0, N_SECTION * 65536).astype(jnp.int32)
    live_batches = jax.random.randint(key_of[7], (1,), 0, 65536 * (MB - MB // 2 + 1)).astype(jnp.int32)
    return dict(section_up=section_up, section_down=section_down, backup_up=backup_up, backup_down=backup_down, norm_gain=norm_gain, micro_batches=micro_batches, failed_section=failed_section, live_batches=live_batches)


def reference(section_up, section_down, backup_up, backup_down, norm_gain, micro_batches, failed_section, live_batches):
    failed = failed_section[0] % N_SECTION
    live_count = MB // 2 + live_batches[0] % (MB - MB // 2 + 1)
    spare_up = backup_up.reshape(D, FF)
    spare_down = backup_down.reshape(D, FF)
    batch_index = lax.broadcasted_iota(jnp.int32, (MB, 1, 1), 0)
    inputs = jnp.where(batch_index < live_count, micro_batches, jnp.zeros_like(micro_batches))
    state_rows = inputs.reshape(MB * TOKENS_MB, D)
    block_width = FF // N_TENSOR

    def one_section(carried, section_layer):
        up_weight, down_weight, gain_row, section_index = section_layer
        chosen_up = jnp.where(section_index == failed, spare_up, up_weight)
        chosen_down = jnp.where(section_index == failed, spare_down, down_weight)
        values = carried.astype(jnp.float32)
        mean_square = lax.optimization_barrier(jnp.mean(values * values, axis=1, keepdims=True))
        normed = (values * lax.rsqrt(mean_square + 1e-05) * gain_row).astype(jnp.bfloat16)
        hidden = jax.nn.silu(jnp.dot(normed, chosen_up, preferred_element_type=jnp.float32)).astype(jnp.bfloat16)
        down_total = jnp.zeros((carried.shape[0], D), jnp.float32)
        for block_index in range(N_TENSOR):
            lower = block_index * block_width
            block_term = lax.dot_general(hidden[:, lower:lower + block_width], chosen_down[:, lower:lower + block_width], (((1,), (1,)), ((), ())), preferred_element_type=jnp.float32)
            down_total = down_total + lax.optimization_barrier(block_term.astype(jnp.bfloat16)).astype(jnp.float32)
        return ((values + down_total).astype(jnp.bfloat16), None)
    indices = jnp.arange(N_SECTION, dtype=jnp.int32)
    final_rows, _ = lax.scan(one_section, state_rows, (section_up, section_down, norm_gain, indices))
    return final_rows.reshape(MB, TOKENS_MB, D)
```

```python
import functools

import jax
import jax.numpy as jnp
from jax import lax
from jax.experimental import pallas as pl
from jax.experimental.pallas import tpu as pltpu
from jax.sharding import PartitionSpec as P

MESH = pl.DeviceIdType.MESH


def relay_kernel(
    sizes,
    inputs_ref,
    gain_ref,
    up_hbm,
    down_hbm,
    finals_ref,
    up,
    down,
    xbuf,
    part_out,
    part_in,
    square_out,
    square_in,
    down_out,
    down_in,
    done_buf,
    fin,
    weight_sem,
    start_send,
    start_recv,
    x_send,
    x_recv,
    part_send,
    part_recv,
    square_send,
    square_recv,
    down_send,
    down_recv,
    fin_send,
    fin_recv,
    fin_self,
):
    S, T, R, chunks, group, tok = sizes
    s, t, d = lax.axis_index("section"), lax.axis_index("tensor"), lax.axis_index("dp")
    rows = group * R * tok
    width = xbuf.shape[-1]
    model = width * T * R
    first, last = s == 0, s == S - 1
    per_section = chunks * group // S

    up_copy = pltpu.make_async_copy(up_hbm, up, weight_sem.at[0])
    down_copy = pltpu.make_async_copy(down_hbm, down, weight_sem.at[1])
    up_copy.start()
    down_copy.start()

    owner = t // (T // R)

    def entering(block, target, how):
        slot = lax.rem(t, T // R) * R + block
        src = inputs_ref.at[:, :, pl.ds(block * width, width)]
        dst = xbuf.at[:, slot, pl.ds(pl.multiple_of(d * tok, tok), tok), :]
        if how == "local":
            return pltpu.make_async_copy(src, dst, start_recv.at[slot, d])
        return pltpu.make_async_remote_copy(
            src, dst, start_send.at[block, target], start_recv.at[slot, d],
            device_id=(s, target, owner), device_id_type=MESH,
        )

    def entering_wait(slot, replica):
        src = inputs_ref.at[:, :, pl.ds(0, width)]
        dst = xbuf.at[:, slot, pl.ds(replica * tok, tok), :]
        pltpu.make_async_copy(src, dst, start_recv.at[slot, replica]).wait()

    @pl.when(first)
    def _():
        for target in range(T):
            for block in range(R):
                mine = (target == t) & (owner == d)

                @pl.when(mine)
                def _():
                    entering(block, target, "local").start()

                @pl.when(jnp.logical_not(mine))
                def _():
                    entering(block, target, "remote").start()

        for slot in range(T):
            for replica in range(R):
                entering_wait(slot, replica)

    def pass_on(c, k):
        target = lax.rem(t + k, T)
        return pltpu.make_async_remote_copy(
            done_buf.at[c], xbuf.at[c, t], x_send.at[c, k], x_recv.at[c, t],
            device_id=(s + 1, target, d), device_id_type=MESH,
        )

    def part_copy(c):
        return pltpu.make_async_remote_copy(
            part_out.at[c], part_in.at[c], part_send.at[c], part_recv.at[c],
            device_id=(s, t, 1 - d), device_id_type=MESH,
        )

    def square_copy(c):
        return pltpu.make_async_remote_copy(
            square_out.at[c], square_in.at[c], square_send.at[c], square_recv.at[c],
            device_id=(s, t, 1 - d), device_id_type=MESH,
        )

    def down_copy_to(c, k):
        target = lax.rem(t + k, T)
        return pltpu.make_async_remote_copy(
            down_out.at[c, k], down_in.at[c, k], down_send.at[c, k], down_recv.at[c, k],
            device_id=(s, target, d), device_id_type=MESH,
        )

    feature_block = d * T + t
    fin_shard, fin_half = feature_block // R, lax.rem(feature_block, R)

    def final_copy(c, g, replica, how):
        batch = c * group + g
        section, slot = batch // per_section, lax.rem(batch, per_section)
        src = done_buf.at[c, pl.ds((g * R + replica) * tok, tok), :]
        dst = fin.at[slot, fin_half]
        sem = fin_recv.at[slot, fin_half]
        if how == "local":
            return section, pltpu.make_async_copy(src, dst, sem)
        return section, pltpu.make_async_remote_copy(
            src, dst, fin_send.at[batch, replica], sem,
            device_id=(section, fin_shard, replica), device_id_type=MESH,
        )

    def is_self(section, replica):
        return (section == s) & (fin_shard == t) & (replica == d)

    def stage_a(c):
        @pl.when(jnp.logical_not(first))
        def _():
            for slot in range(T):
                pltpu.make_async_copy(done_buf.at[c], xbuf.at[c, slot], x_recv.at[c, slot]).wait()

        total = jnp.zeros((rows, 1), jnp.float32)
        pieces = []
        for slot in range(T):
            values = xbuf[c, slot].astype(jnp.float32)
            total = total + jnp.sum(values * values, axis=1, keepdims=True)
            pieces.append((values * gain_ref[:, pl.ds(slot * width, width)]).astype(jnp.bfloat16))
        square_out[c] = jnp.broadcast_to(total, square_out.shape[1:])
        square_copy(c).start()
        scaled = jnp.concatenate(pieces, axis=1)
        part_out[c] = jnp.dot(scaled, up[...], preferred_element_type=jnp.float32).astype(jnp.bfloat16)
        part_copy(c).start()

    def stage_b(c):
        square_copy(c).wait_recv()
        part_copy(c).wait_recv()
        mean_square = (square_out[c][:, :1] + square_in[c][:, :1]) * (1.0 / model)
        pre = part_out[c].astype(jnp.float32) + part_in[c].astype(jnp.float32)
        pre = pre * lax.rsqrt(mean_square + 1e-05)
        hidden = (pre / (1.0 + jnp.exp(-pre))).astype(jnp.bfloat16)
        for k in (2, 1, 3, 0) if T == 4 else tuple(range(T - 1, -1, -1)):
            target = lax.rem(t + k, T)
            block = down[pl.ds(pl.multiple_of(target * width, width), width), :]
            down_out[c, k] = lax.dot_general(
                hidden, block, (((1,), (1,)), ((), ())), preferred_element_type=jnp.float32
            ).astype(jnp.bfloat16)
            if k:
                down_copy_to(c, k).start()

    def stage_c(c):
        acc = xbuf[c, t].astype(jnp.float32) + down_out[c, 0].astype(jnp.float32)
        for k in range(1, T):
            down_copy_to(c, k).wait_recv()
            acc = acc + down_in[c, k].astype(jnp.float32)
        done_buf[c] = acc.astype(jnp.bfloat16)

        @pl.when(jnp.logical_not(last))
        def _():
            for k in range(T):
                pass_on(c, k).start()

        @pl.when(last)
        def _():
            for g in range(group):
                for replica in range(R):
                    section, local = final_copy(c, g, replica, "local")
                    _, remote = final_copy(c, g, replica, "remote")
                    mine = is_self(section, replica)

                    @pl.when(mine)
                    def _():
                        local.start()

                    @pl.when(jnp.logical_not(mine))
                    def _():
                        remote.start()

    up_copy.wait()
    down_copy.wait()

    def step(i, _):
        @pl.when(i < chunks)
        def _():
            stage_a(i)

        @pl.when((i >= 1) & (i < chunks + 1))
        def _():
            stage_b(i - 1)

        @pl.when(i >= 2)
        def _():
            stage_c(i - 2)

        return 0

    lax.fori_loop(0, chunks + 2, step, 0)

    for slot in range(per_section):
        for half in range(R):
            pltpu.make_async_copy(
                done_buf.at[0, pl.ds(0, tok), :], fin.at[slot, half], fin_recv.at[slot, half]
            ).wait()
            finals_ref[slot, :, pl.ds(half * width, width)] = fin[slot, half]

    @pl.when(first)
    def _():
        for target in range(T):
            for block in range(R):

                @pl.when(jnp.logical_not((target == t) & (owner == d)))
                def _():
                    entering(block, target, "remote").wait_send()

    def drain(c, _):
        square_copy(c).wait_send()
        part_copy(c).wait_send()
        for k in range(1, T):
            down_copy_to(c, k).wait_send()

        @pl.when(jnp.logical_not(last))
        def _():
            for k in range(T):
                pass_on(c, k).wait_send()

        @pl.when(last)
        def _():
            for g in range(group):
                for replica in range(R):
                    section, remote = final_copy(c, g, replica, "remote")

                    @pl.when(jnp.logical_not(is_self(section, replica)))
                    def _():
                        remote.wait_send()

        return 0

    lax.fori_loop(0, chunks, drain, 0)


def relay(entering, gain, up, down, S, T, R, chunks):
    batches, tok, share = entering.shape
    group = batches // chunks
    rows = group * R * tok
    width = share // R
    wide = up.shape[1]
    bf16, f32 = jnp.bfloat16, jnp.float32
    dma = pltpu.SemaphoreType.DMA
    vmem = pl.BlockSpec(memory_space=pltpu.VMEM)
    hbm = pl.BlockSpec(memory_space=pl.ANY)
    return pl.pallas_call(
        functools.partial(relay_kernel, (S, T, R, chunks, group, tok)),
        out_shape=jax.ShapeDtypeStruct((batches // S, tok, share), bf16),
        in_specs=[vmem, vmem, hbm, hbm],
        out_specs=vmem,
        scratch_shapes=[
            pltpu.VMEM(up.shape, bf16),
            pltpu.VMEM(down.shape, bf16),
            pltpu.VMEM((chunks, T, rows, width), bf16),
            pltpu.VMEM((chunks, rows, wide), bf16),
            pltpu.VMEM((chunks, rows, wide), bf16),
            pltpu.VMEM((chunks, rows, 128), f32),
            pltpu.VMEM((chunks, rows, 128), f32),
            pltpu.VMEM((chunks, T, rows, width), bf16),
            pltpu.VMEM((chunks, T, rows, width), bf16),
            pltpu.VMEM((chunks, rows, width), bf16),
            pltpu.VMEM((batches // S, R, tok, width), bf16),
            dma((2,)),
            dma((R, T)),
            dma((T, R)),
            dma((chunks, T)),
            dma((chunks, T)),
            dma((chunks,)),
            dma((chunks,)),
            dma((chunks,)),
            dma((chunks,)),
            dma((chunks, T)),
            dma((chunks, T)),
            dma((batches, R)),
            dma((batches // S, R)),
            dma((1,)),
        ],
        compiler_params=pltpu.CompilerParams(has_side_effects=True, vmem_limit_bytes=60 * 1024 * 1024),
    )(entering, gain, up, down)


def body(
    section_up,
    section_down,
    backup_up,
    backup_down,
    norm_gain,
    micro_batches,
    failed_section,
    live_batches,
):
    S, T, R = lax.axis_size("section"), lax.axis_size("tensor"), lax.axis_size("dp")
    section_number = lax.axis_index("section")
    is_failed = section_number == failed_section[0] % S
    block_width = section_up.shape[2]

    def rebuilt(backup, own):
        pieces = lax.all_to_all(backup, "tensor", split_axis=4, concat_axis=2, tiled=True)
        gathered = lax.all_gather(pieces, "section", axis=1, tiled=True)
        return jnp.where(is_failed, gathered.reshape(-1, block_width), own)

    mine_up = rebuilt(backup_up, section_up[0])
    mine_down = rebuilt(backup_down, section_down[0])
    batch_count = micro_batches.shape[0]
    live_count = batch_count // 2 + live_batches[0] % (batch_count - batch_count // 2 + 1)
    alive = lax.broadcasted_iota(jnp.int32, (batch_count, 1, 1), 0) < live_count
    entering = jnp.where(alive, micro_batches, jnp.zeros_like(micro_batches))
    depth = section_up.shape[1]
    gain = lax.dynamic_slice_in_dim(norm_gain, lax.axis_index("dp") * depth, depth, 1)
    return relay(entering, gain, mine_up, mine_down, S, T, R, batch_count)


def solution(mesh):
    placed = (
        P("section", "dp", "tensor"),
        P("section", "dp", "tensor"),
        P("dp", "section", "tensor", None, None),
        P("dp", "section", "tensor", None, None),
        P("section", None),
        P(None, "dp", "tensor"),
        P(),
        P(),
    )
    return jax.shard_map(
        body, mesh=mesh, in_specs=placed, out_specs=P("section", "dp", "tensor"), check_vma=False
    )
```

```python
import functools

import jax
import jax.numpy as jnp
from jax import lax
from jax.experimental import pallas as pl
from jax.experimental.pallas import tpu as pltpu
from jax.sharding import PartitionSpec as P

MESH = pl.DeviceIdType.MESH


def relay_kernel(
    sizes,
    failed,
    inputs_ref,
    gain_ref,
    up_hbm,
    down_hbm,
    spare_up,
    spare_down,
    finals_ref,
    up,
    down,
    xbuf,
    part_out,
    part_in,
    square_out,
    square_in,
    down_out,
    down_in,
    done_buf,
    fin,
    staged,
    weight_sem,
    spread_send,
    spread_recv,
    piece_send,
    piece_recv,
    start_send,
    start_recv,
    x_send,
    x_recv,
    part_send,
    part_recv,
    square_send,
    square_recv,
    down_send,
    down_recv,
    fin_send,
    fin_recv,
):
    S, T, R, chunks, group, tok = sizes
    s, t, d = lax.axis_index("section"), lax.axis_index("tensor"), lax.axis_index("dp")
    rows = group * R * tok
    width = xbuf.shape[-1]
    model = width * T * R
    first, last = s == 0, s == S - 1
    per_section = chunks * group // S

    is_failed = s == failed
    up_copy = pltpu.make_async_copy(up_hbm, up, weight_sem.at[0])
    down_copy = pltpu.make_async_copy(down_hbm, down, weight_sem.at[1])
    spares, chosen = (spare_up, spare_down), (up, down)
    piece, wide = spare_up.shape[0], up.shape[1]
    moves = [(matrix, k) for matrix in range(2) for k in range(1, T)]

    def columns(matrix, target):
        return spares[matrix].at[:, pl.ds(pl.multiple_of(target * wide, wide), wide)]

    def place(matrix, section, shard):
        start = pl.multiple_of((section * T + shard) * piece, piece)
        return chosen[matrix].at[pl.ds(start, piece), :]

    def spread(matrix, k, landed):
        target = lax.rem(t + k, T)
        dst = place(matrix, s, t) if landed else staged.at[matrix, k]
        sem = piece_recv.at[matrix, s * T + t] if landed else spread_recv.at[matrix, k]
        return pltpu.make_async_remote_copy(
            columns(matrix, target), dst, spread_send.at[matrix, k], sem,
            device_id=(s, target, d), device_id_type=MESH,
        )

    def forward(matrix, k):
        source = lax.rem(t + T - k, T)
        src = staged.at[matrix, k] if k else columns(matrix, t)
        return pltpu.make_async_remote_copy(
            src, place(matrix, s, source), piece_send.at[matrix, k], piece_recv.at[matrix, s * T + source],
            device_id=(failed, t, d), device_id_type=MESH,
        )

    def own_piece(matrix):
        return pltpu.make_async_copy(
            columns(matrix, t), place(matrix, s, t), piece_recv.at[matrix, s * T + t]
        )

    def relay_piece(p):
        matrix, k = moves[p]
        spread(matrix, k, False).wait_recv()
        forward(matrix, k).start()

    @pl.when(is_failed)
    def _():
        for matrix in range(2):
            own_piece(matrix).start()
            for k in range(1, T):
                spread(matrix, k, True).start()

    @pl.when(jnp.logical_not(is_failed))
    def _():
        up_copy.start()
        down_copy.start()
        for matrix in range(2):
            forward(matrix, 0).start()
            for k in range(1, T):
                spread(matrix, k, False).start()

    def weights_ready(matrix):
        @pl.when(is_failed)
        def _():
            def one(i, _):
                section, shard = i // T, lax.rem(i, T)
                pltpu.make_async_copy(
                    columns(matrix, t), place(matrix, section, shard), piece_recv.at[matrix, i]
                ).wait()
                return 0

            lax.fori_loop(0, S * T, one, 0)

        @pl.when(jnp.logical_not(is_failed))
        def _():
            (up_copy, down_copy)[matrix].wait()

    owner = t // (T // R)

    def entering(block, target, how):
        slot = lax.rem(t, T // R) * R + block
        src = inputs_ref.at[:, :, pl.ds(block * width, width)]
        dst = xbuf.at[:, slot, pl.ds(pl.multiple_of(d * tok, tok), tok), :]
        if how == "local":
            return pltpu.make_async_copy(src, dst, start_recv.at[slot, d])
        return pltpu.make_async_remote_copy(
            src, dst, start_send.at[block, target], start_recv.at[slot, d],
            device_id=(s, target, owner), device_id_type=MESH,
        )

    def entering_wait(slot, replica):
        src = inputs_ref.at[:, :, pl.ds(0, width)]
        dst = xbuf.at[:, slot, pl.ds(replica * tok, tok), :]
        pltpu.make_async_copy(src, dst, start_recv.at[slot, replica]).wait()

    @pl.when(first)
    def _():
        for target in range(T):
            for block in range(R):
                mine = (target == t) & (owner == d)

                @pl.when(mine)
                def _():
                    entering(block, target, "local").start()

                @pl.when(jnp.logical_not(mine))
                def _():
                    entering(block, target, "remote").start()

        for slot in range(T):
            for replica in range(R):
                entering_wait(slot, replica)

    def pass_on(c, k):
        target = lax.rem(t + k, T)
        return pltpu.make_async_remote_copy(
            done_buf.at[c], xbuf.at[c, t], x_send.at[c, k], x_recv.at[c, t],
            device_id=(s + 1, target, d), device_id_type=MESH,
        )

    def part_copy(c):
        return pltpu.make_async_remote_copy(
            part_out.at[c], part_in.at[c], part_send.at[c], part_recv.at[c],
            device_id=(s, t, 1 - d), device_id_type=MESH,
        )

    def square_copy(c):
        return pltpu.make_async_remote_copy(
            square_out.at[c], square_in.at[c], square_send.at[c], square_recv.at[c],
            device_id=(s, t, 1 - d), device_id_type=MESH,
        )

    def down_copy_to(c, k):
        target = lax.rem(t + k, T)
        return pltpu.make_async_remote_copy(
            down_out.at[c, k], down_in.at[c, k], down_send.at[c, k], down_recv.at[c, k],
            device_id=(s, target, d), device_id_type=MESH,
        )

    feature_block = d * T + t
    fin_shard, fin_half = feature_block // R, lax.rem(feature_block, R)

    def final_copy(c, g, replica, how):
        batch = c * group + g
        section, slot = batch // per_section, lax.rem(batch, per_section)
        src = done_buf.at[c, pl.ds((g * R + replica) * tok, tok), :]
        dst = fin.at[slot, fin_half]
        sem = fin_recv.at[slot, fin_half]
        if how == "local":
            return section, pltpu.make_async_copy(src, dst, sem)
        return section, pltpu.make_async_remote_copy(
            src, dst, fin_send.at[batch, replica], sem,
            device_id=(section, fin_shard, replica), device_id_type=MESH,
        )

    def is_self(section, replica):
        return (section == s) & (fin_shard == t) & (replica == d)

    def stage_a(c):
        @pl.when(jnp.logical_not(first))
        def _():
            for slot in range(T):
                pltpu.make_async_copy(done_buf.at[c], xbuf.at[c, slot], x_recv.at[c, slot]).wait()

        total = jnp.zeros((rows, 1), jnp.float32)
        pieces = []
        for slot in range(T):
            values = xbuf[c, slot].astype(jnp.float32)
            total = total + jnp.sum(values * values, axis=1, keepdims=True)
            pieces.append((values * gain_ref[:, pl.ds(slot * width, width)]).astype(jnp.bfloat16))
        square_out[c] = jnp.broadcast_to(total, square_out.shape[1:])
        square_copy(c).start()
        scaled = jnp.concatenate(pieces, axis=1)
        part_out[c] = jnp.dot(scaled, up[...], preferred_element_type=jnp.float32).astype(jnp.bfloat16)
        part_copy(c).start()

    def stage_b(c):
        square_copy(c).wait_recv()
        part_copy(c).wait_recv()
        mean_square = (square_out[c][:, :1] + square_in[c][:, :1]) * (1.0 / model)
        pre = part_out[c].astype(jnp.float32) + part_in[c].astype(jnp.float32)
        pre = pre * lax.rsqrt(mean_square + 1e-05)
        hidden = (pre / (1.0 + jnp.exp(-pre))).astype(jnp.bfloat16)
        for k in (2, 1, 3, 0) if T == 4 else tuple(range(T - 1, -1, -1)):
            target = lax.rem(t + k, T)
            block = down[pl.ds(pl.multiple_of(target * width, width), width), :]
            down_out[c, k] = lax.dot_general(
                hidden, block, (((1,), (1,)), ((), ())), preferred_element_type=jnp.float32
            ).astype(jnp.bfloat16)
            if k:
                down_copy_to(c, k).start()

    def stage_c(c):
        acc = xbuf[c, t].astype(jnp.float32) + down_out[c, 0].astype(jnp.float32)
        for k in range(1, T):
            down_copy_to(c, k).wait_recv()
            acc = acc + down_in[c, k].astype(jnp.float32)
        done_buf[c] = acc.astype(jnp.bfloat16)

        @pl.when(jnp.logical_not(last))
        def _():
            for k in range(T):
                pass_on(c, k).start()

        @pl.when(last)
        def _():
            for g in range(group):
                for replica in range(R):
                    section, local = final_copy(c, g, replica, "local")
                    _, remote = final_copy(c, g, replica, "remote")
                    mine = is_self(section, replica)

                    @pl.when(mine)
                    def _():
                        local.start()

                    @pl.when(jnp.logical_not(mine))
                    def _():
                        remote.start()

    early = 2 * s
    for p in range(len(moves)):

        @pl.when((s > failed) | ((s < failed) & (p < early)))
        def _():
            relay_piece(p)

    def step(i, _):
        @pl.when(i == 0)
        def _():
            weights_ready(0)

        @pl.when(i == 1)
        def _():
            weights_ready(1)

        @pl.when(i < chunks)
        def _():
            stage_a(i)

        @pl.when((i >= 1) & (i < chunks + 1))
        def _():
            stage_b(i - 1)

        @pl.when(i >= 2)
        def _():
            stage_c(i - 2)

        for p in range(len(moves)):

            @pl.when((s < failed) & (i + early == p))
            def _():
                relay_piece(p)

        return 0

    lax.fori_loop(0, chunks + 2, step, 0)
    for p in range(len(moves)):

        @pl.when((s < failed) & (p >= early + chunks + 2))
        def _():
            relay_piece(p)

    for slot in range(per_section):
        for half in range(R):
            pltpu.make_async_copy(
                done_buf.at[0, pl.ds(0, tok), :], fin.at[slot, half], fin_recv.at[slot, half]
            ).wait()
            finals_ref[slot, :, pl.ds(half * width, width)] = fin[slot, half]

    @pl.when(is_failed)
    def _():
        for matrix, k in moves:
            spread(matrix, k, True).wait_send()

    @pl.when(jnp.logical_not(is_failed))
    def _():
        for matrix in range(2):
            forward(matrix, 0).wait_send()
        for matrix, k in moves:
            spread(matrix, k, False).wait_send()
            forward(matrix, k).wait_send()

    @pl.when(first)
    def _():
        for target in range(T):
            for block in range(R):

                @pl.when(jnp.logical_not((target == t) & (owner == d)))
                def _():
                    entering(block, target, "remote").wait_send()

    def drain(c, _):
        square_copy(c).wait_send()
        part_copy(c).wait_send()
        for k in range(1, T):
            down_copy_to(c, k).wait_send()

        @pl.when(jnp.logical_not(last))
        def _():
            for k in range(T):
                pass_on(c, k).wait_send()

        @pl.when(last)
        def _():
            for g in range(group):
                for replica in range(R):
                    section, remote = final_copy(c, g, replica, "remote")

                    @pl.when(jnp.logical_not(is_self(section, replica)))
                    def _():
                        remote.wait_send()

        return 0

    lax.fori_loop(0, chunks, drain, 0)


def relay(entering, gain, up, down, spare_up, spare_down, S, T, R, chunks, failed):
    batches, tok, share = entering.shape
    group = batches // chunks
    rows = group * R * tok
    width = share // R
    wide = up.shape[1]
    bf16, f32 = jnp.bfloat16, jnp.float32
    dma = pltpu.SemaphoreType.DMA
    vmem = pl.BlockSpec(memory_space=pltpu.VMEM)
    hbm = pl.BlockSpec(memory_space=pl.ANY)
    return pl.pallas_call(
        functools.partial(relay_kernel, (S, T, R, chunks, group, tok), failed),
        out_shape=jax.ShapeDtypeStruct((batches // S, tok, share), bf16),
        in_specs=[vmem, vmem, hbm, hbm, hbm, hbm],
        out_specs=vmem,
        scratch_shapes=[
            pltpu.VMEM(up.shape, bf16),
            pltpu.VMEM(down.shape, bf16),
            pltpu.VMEM((chunks, T, rows, width), bf16),
            pltpu.VMEM((chunks, rows, wide), bf16),
            pltpu.VMEM((chunks, rows, wide), bf16),
            pltpu.VMEM((chunks, rows, 128), f32),
            pltpu.VMEM((chunks, rows, 128), f32),
            pltpu.VMEM((chunks, T, rows, width), bf16),
            pltpu.VMEM((chunks, T, rows, width), bf16),
            pltpu.VMEM((chunks, rows, width), bf16),
            pltpu.VMEM((batches // S, R, tok, width), bf16),
            pltpu.VMEM((2, T, spare_up.shape[0], wide), bf16),
            dma((2,)),
            dma((2, T)),
            dma((2, T)),
            dma((2, T)),
            dma((2, S * T)),
            dma((R, T)),
            dma((T, R)),
            dma((chunks, T)),
            dma((chunks, T)),
            dma((chunks,)),
            dma((chunks,)),
            dma((chunks,)),
            dma((chunks,)),
            dma((chunks, T)),
            dma((chunks, T)),
            dma((batches, R)),
            dma((batches // S, R)),
        ],
        compiler_params=pltpu.CompilerParams(has_side_effects=True, vmem_limit_bytes=60 * 1024 * 1024),
    )(entering, gain, up, down, spare_up, spare_down)


def body(
    section_up,
    section_down,
    backup_up,
    backup_down,
    norm_gain,
    micro_batches,
    failed_section,
    live_batches,
):
    S, T, R = lax.axis_size("section"), lax.axis_size("tensor"), lax.axis_size("dp")
    batch_count = micro_batches.shape[0]
    live_count = batch_count // 2 + live_batches[0] % (batch_count - batch_count // 2 + 1)
    alive = lax.broadcasted_iota(jnp.int32, (batch_count, 1, 1), 0) < live_count
    entering = jnp.where(alive, micro_batches, jnp.zeros_like(micro_batches))
    depth = section_up.shape[1]
    gain = lax.dynamic_slice_in_dim(norm_gain, lax.axis_index("dp") * depth, depth, 1)
    operands = (
        entering,
        gain,
        section_up[0],
        section_down[0],
        backup_up.reshape(backup_up.shape[3:]),
        backup_down.reshape(backup_down.shape[3:]),
    )

    def with_failed(failed):
        return lambda *arrays: relay(*arrays, S, T, R, batch_count, failed)

    return lax.switch(failed_section[0] % S, [with_failed(f) for f in range(S)], *operands)


def solution(mesh):
    placed = (
        P("section", "dp", "tensor"),
        P("section", "dp", "tensor"),
        P("dp", "section", "tensor", None, None),
        P("dp", "section", "tensor", None, None),
        P("section", None),
        P(None, "dp", "tensor"),
        P(),
        P(),
    )
    return jax.shard_map(
        body, mesh=mesh, in_specs=placed, out_specs=P("section", "dp", "tensor"), check_vma=False
    )
```

```python
import functools

import jax
import jax.numpy as jnp
from jax import lax
from jax.experimental import pallas as pl
from jax.experimental.pallas import tpu as pltpu
from jax.sharding import PartitionSpec as P

MESH = pl.DeviceIdType.MESH


def relay_kernel(
    sizes,
    failed,
    inputs_ref,
    gain_ref,
    up_hbm,
    down_hbm,
    spare_up,
    spare_down,
    finals_ref,
    up,
    down,
    xbuf,
    part_out,
    part_in,
    square_out,
    square_in,
    down_out,
    down_in,
    done_buf,
    fin,
    staged,
    weight_sem,
    spread_send,
    spread_recv,
    piece_send,
    piece_recv,
    start_send,
    start_recv,
    x_send,
    x_recv,
    part_send,
    part_recv,
    square_send,
    square_recv,
    down_send,
    down_recv,
    fin_send,
    fin_recv,
):
    S, T, R, chunks, group, tok = sizes
    s, t, d = lax.axis_index("section"), lax.axis_index("tensor"), lax.axis_index("dp")
    rows = group * R * tok
    width = xbuf.shape[-1]
    model = width * T * R
    first, last = s == 0, s == S - 1
    per_section = finals_ref.shape[0]

    is_failed = s == failed
    up_copy = pltpu.make_async_copy(up_hbm, up, weight_sem.at[0])
    down_copy = pltpu.make_async_copy(down_hbm, down, weight_sem.at[1])
    spares, chosen = (spare_up, spare_down), (up, down)
    piece, wide = spare_up.shape[0], up.shape[1]
    moves = [(matrix, k) for matrix in range(2) for k in range(1, T)]

    def columns(matrix, target):
        return spares[matrix].at[:, pl.ds(pl.multiple_of(target * wide, wide), wide)]

    def place(matrix, section, shard):
        start = pl.multiple_of((section * T + shard) * piece, piece)
        return chosen[matrix].at[pl.ds(start, piece), :]

    def spread(matrix, k, landed):
        target = lax.rem(t + k, T)
        dst = place(matrix, s, t) if landed else staged.at[matrix, k]
        sem = piece_recv.at[matrix, s * T + t] if landed else spread_recv.at[matrix, k]
        return pltpu.make_async_remote_copy(
            columns(matrix, target), dst, spread_send.at[matrix, k], sem,
            device_id=(s, target, d), device_id_type=MESH,
        )

    def forward(matrix, k):
        source = lax.rem(t + T - k, T)
        src = staged.at[matrix, k] if k else columns(matrix, t)
        return pltpu.make_async_remote_copy(
            src, place(matrix, s, source), piece_send.at[matrix, k], piece_recv.at[matrix, s * T + source],
            device_id=(failed, t, d), device_id_type=MESH,
        )

    def own_piece(matrix):
        return pltpu.make_async_copy(
            columns(matrix, t), place(matrix, s, t), piece_recv.at[matrix, s * T + t]
        )

    def relay_piece(p):
        matrix, k = moves[p]
        spread(matrix, k, False).wait_recv()
        forward(matrix, k).start()

    @pl.when(is_failed)
    def _():
        for matrix in range(2):
            own_piece(matrix).start()
            for k in range(1, T):
                spread(matrix, k, True).start()

    @pl.when(jnp.logical_not(is_failed))
    def _():
        up_copy.start()
        down_copy.start()
        for matrix in range(2):
            forward(matrix, 0).start()
            for k in range(1, T):
                spread(matrix, k, False).start()

    def weights_ready(matrix):
        @pl.when(is_failed)
        def _():
            def one(i, _):
                section, shard = i // T, lax.rem(i, T)
                pltpu.make_async_copy(
                    columns(matrix, t), place(matrix, section, shard), piece_recv.at[matrix, i]
                ).wait()
                return 0

            lax.fori_loop(0, S * T, one, 0)

        @pl.when(jnp.logical_not(is_failed))
        def _():
            (up_copy, down_copy)[matrix].wait()

    owner = t // (T // R)

    def entering(block, target, how):
        slot = lax.rem(t, T // R) * R + block
        src = inputs_ref.at[pl.ds(0, chunks * group), :, pl.ds(block * width, width)]
        dst = xbuf.at[:, slot, pl.ds(pl.multiple_of(d * tok, tok), tok), :]
        if how == "local":
            return pltpu.make_async_copy(src, dst, start_recv.at[slot, d])
        return pltpu.make_async_remote_copy(
            src, dst, start_send.at[block, target], start_recv.at[slot, d],
            device_id=(s, target, owner), device_id_type=MESH,
        )

    def entering_wait(slot, replica):
        src = inputs_ref.at[pl.ds(0, chunks * group), :, pl.ds(0, width)]
        dst = xbuf.at[:, slot, pl.ds(replica * tok, tok), :]
        pltpu.make_async_copy(src, dst, start_recv.at[slot, replica]).wait()

    @pl.when(first)
    def _():
        for target in range(T):
            for block in range(R):
                mine = (target == t) & (owner == d)

                @pl.when(mine)
                def _():
                    entering(block, target, "local").start()

                @pl.when(jnp.logical_not(mine))
                def _():
                    entering(block, target, "remote").start()

        for slot in range(T):
            for replica in range(R):
                entering_wait(slot, replica)

    def pass_on(c, k):
        target = lax.rem(t + k, T)
        return pltpu.make_async_remote_copy(
            done_buf.at[c], xbuf.at[c, t], x_send.at[c, k], x_recv.at[c, t],
            device_id=(s + 1, target, d), device_id_type=MESH,
        )

    def part_copy(c):
        return pltpu.make_async_remote_copy(
            part_out.at[c], part_in.at[c], part_send.at[c], part_recv.at[c],
            device_id=(s, t, 1 - d), device_id_type=MESH,
        )

    def square_copy(c):
        return pltpu.make_async_remote_copy(
            square_out.at[c], square_in.at[c], square_send.at[c], square_recv.at[c],
            device_id=(s, t, 1 - d), device_id_type=MESH,
        )

    def down_copy_to(c, k):
        target = lax.rem(t + k, T)
        return pltpu.make_async_remote_copy(
            down_out.at[c, k], down_in.at[c, k], down_send.at[c, k], down_recv.at[c, k],
            device_id=(s, target, d), device_id_type=MESH,
        )

    feature_block = d * T + t
    fin_shard, fin_half = feature_block // R, lax.rem(feature_block, R)

    def final_copy(c, g, replica, how):
        batch = c * group + g
        section, slot = batch // per_section, lax.rem(batch, per_section)
        src = done_buf.at[c, pl.ds((g * R + replica) * tok, tok), :]
        dst = fin.at[slot, fin_half]
        sem = fin_recv.at[slot, fin_half]
        if how == "local":
            return section, pltpu.make_async_copy(src, dst, sem)
        return section, pltpu.make_async_remote_copy(
            src, dst, fin_send.at[batch, replica], sem,
            device_id=(section, fin_shard, replica), device_id_type=MESH,
        )

    def is_self(section, replica):
        return (section == s) & (fin_shard == t) & (replica == d)

    def stage_a(c):
        @pl.when(jnp.logical_not(first))
        def _():
            for slot in range(T):
                pltpu.make_async_copy(done_buf.at[c], xbuf.at[c, slot], x_recv.at[c, slot]).wait()

        total = jnp.zeros((rows, 1), jnp.float32)
        pieces = []
        for slot in range(T):
            values = xbuf[c, slot].astype(jnp.float32)
            total = total + jnp.sum(values * values, axis=1, keepdims=True)
            pieces.append((values * gain_ref[:, pl.ds(slot * width, width)]).astype(jnp.bfloat16))
        square_out[c] = jnp.broadcast_to(total, square_out.shape[1:])
        square_copy(c).start()
        scaled = jnp.concatenate(pieces, axis=1)
        part_out[c] = jnp.dot(scaled, up[...], preferred_element_type=jnp.float32).astype(jnp.bfloat16)
        part_copy(c).start()

    def stage_b(c):
        square_copy(c).wait_recv()
        part_copy(c).wait_recv()
        mean_square = (square_out[c][:, :1] + square_in[c][:, :1]) * (1.0 / model)
        pre = part_out[c].astype(jnp.float32) + part_in[c].astype(jnp.float32)
        pre = pre * lax.rsqrt(mean_square + 1e-05)
        hidden = (pre / (1.0 + jnp.exp(-pre))).astype(jnp.bfloat16)

        def block_sum(i, _):
            k = lax.rem(i + 1, T)
            target = lax.rem(t + k, T)
            block = down[pl.ds(pl.multiple_of(target * width, width), width), :]
            down_out[c, k] = lax.dot_general(
                hidden, block, (((1,), (1,)), ((), ())), preferred_element_type=jnp.float32
            ).astype(jnp.bfloat16)

            @pl.when(k > 0)
            def _():
                down_copy_to(c, k).start()

            return 0

        lax.fori_loop(0, T, block_sum, 0)

    def stage_c(c):
        acc = xbuf[c, t].astype(jnp.float32) + down_out[c, 0].astype(jnp.float32)
        for k in range(1, T):
            down_copy_to(c, k).wait_recv()
            acc = acc + down_in[c, k].astype(jnp.float32)
        done_buf[c] = acc.astype(jnp.bfloat16)

        @pl.when(jnp.logical_not(last))
        def _():
            for k in range(T):
                pass_on(c, k).start()

        @pl.when(last)
        def _():
            for g in range(group):
                for replica in range(R):
                    section, local = final_copy(c, g, replica, "local")
                    _, remote = final_copy(c, g, replica, "remote")
                    mine = is_self(section, replica)

                    @pl.when(mine)
                    def _():
                        local.start()

                    @pl.when(jnp.logical_not(mine))
                    def _():
                        remote.start()

    early = 2 * s
    for p in range(len(moves)):

        @pl.when((s > failed) | ((s < failed) & (p < early)))
        def _():
            relay_piece(p)

    def step(i, _):
        @pl.when(i == 0)
        def _():
            weights_ready(0)

        @pl.when(i == 1)
        def _():
            weights_ready(1)

        @pl.when(i < chunks)
        def _():
            stage_a(i)

        @pl.when((i >= 1) & (i < chunks + 1))
        def _():
            stage_b(i - 1)

        @pl.when(i >= 2)
        def _():
            stage_c(i - 2)

        for p in range(len(moves)):

            @pl.when((s < failed) & (i + early == p))
            def _():
                relay_piece(p)

        return 0

    lax.fori_loop(0, chunks + 2, step, 0)
    for p in range(len(moves)):

        @pl.when((s < failed) & (p >= early + chunks + 2))
        def _():
            relay_piece(p)

    for slot in range(per_section):
        runs = s * per_section + slot < chunks * group

        @pl.when(runs)
        def _():
            for half in range(R):
                pltpu.make_async_copy(
                    done_buf.at[0, pl.ds(0, tok), :], fin.at[slot, half], fin_recv.at[slot, half]
                ).wait()
                finals_ref[slot, :, pl.ds(half * width, width)] = fin[slot, half]

        @pl.when(jnp.logical_not(runs))
        def _():
            finals_ref[slot] = jnp.zeros(finals_ref.shape[1:], finals_ref.dtype)

    @pl.when(is_failed)
    def _():
        for matrix, k in moves:
            spread(matrix, k, True).wait_send()

    @pl.when(jnp.logical_not(is_failed))
    def _():
        for matrix in range(2):
            forward(matrix, 0).wait_send()
        for matrix, k in moves:
            spread(matrix, k, False).wait_send()
            forward(matrix, k).wait_send()

    @pl.when(first)
    def _():
        for target in range(T):
            for block in range(R):

                @pl.when(jnp.logical_not((target == t) & (owner == d)))
                def _():
                    entering(block, target, "remote").wait_send()

    def drain(c, _):
        square_copy(c).wait_send()
        part_copy(c).wait_send()
        for k in range(1, T):
            down_copy_to(c, k).wait_send()

        @pl.when(jnp.logical_not(last))
        def _():
            for k in range(T):
                pass_on(c, k).wait_send()

        @pl.when(last)
        def _():
            for g in range(group):
                for replica in range(R):
                    section, remote = final_copy(c, g, replica, "remote")

                    @pl.when(jnp.logical_not(is_self(section, replica)))
                    def _():
                        remote.wait_send()

        return 0

    lax.fori_loop(0, chunks, drain, 0)


def relay(entering, gain, up, down, spare_up, spare_down, S, T, R, chunks, failed):
    batches, tok, share = entering.shape
    group = 1
    rows = group * R * tok
    width = share // R
    wide = up.shape[1]
    bf16, f32 = jnp.bfloat16, jnp.float32
    dma = pltpu.SemaphoreType.DMA
    vmem = pl.BlockSpec(memory_space=pltpu.VMEM)
    hbm = pl.BlockSpec(memory_space=pl.ANY)
    return pl.pallas_call(
        functools.partial(relay_kernel, (S, T, R, chunks, group, tok), failed),
        out_shape=jax.ShapeDtypeStruct((batches // S, tok, share), bf16),
        in_specs=[vmem, vmem, hbm, hbm, hbm, hbm],
        out_specs=vmem,
        scratch_shapes=[
            pltpu.VMEM(up.shape, bf16),
            pltpu.VMEM(down.shape, bf16),
            pltpu.VMEM((chunks, T, rows, width), bf16),
            pltpu.VMEM((chunks, rows, wide), bf16),
            pltpu.VMEM((chunks, rows, wide), bf16),
            pltpu.VMEM((chunks, rows, 128), f32),
            pltpu.VMEM((chunks, rows, 128), f32),
            pltpu.VMEM((chunks, T, rows, width), bf16),
            pltpu.VMEM((chunks, T, rows, width), bf16),
            pltpu.VMEM((chunks, rows, width), bf16),
            pltpu.VMEM((batches // S, R, tok, width), bf16),
            pltpu.VMEM((2, T, spare_up.shape[0], wide), bf16),
            dma((2,)),
            dma((2, T)),
            dma((2, T)),
            dma((2, T)),
            dma((2, S * T)),
            dma((R, T)),
            dma((T, R)),
            dma((chunks, T)),
            dma((chunks, T)),
            dma((chunks,)),
            dma((chunks,)),
            dma((chunks,)),
            dma((chunks,)),
            dma((chunks, T)),
            dma((chunks, T)),
            dma((batches, R)),
            dma((batches // S, R)),
        ],
        compiler_params=pltpu.CompilerParams(has_side_effects=True, vmem_limit_bytes=60 * 1024 * 1024),
    )(entering, gain, up, down, spare_up, spare_down)


def body(
    section_up,
    section_down,
    backup_up,
    backup_down,
    norm_gain,
    micro_batches,
    failed_section,
    live_batches,
):
    S, T, R = lax.axis_size("section"), lax.axis_size("tensor"), lax.axis_size("dp")
    batch_count = micro_batches.shape[0]
    live_count = batch_count // 2 + live_batches[0] % (batch_count - batch_count // 2 + 1)
    alive = lax.broadcasted_iota(jnp.int32, (batch_count, 1, 1), 0) < live_count
    entering = jnp.where(alive, micro_batches, jnp.zeros_like(micro_batches))
    depth = section_up.shape[1]
    gain = lax.dynamic_slice_in_dim(norm_gain, lax.axis_index("dp") * depth, depth, 1)
    operands = (
        entering,
        gain,
        section_up[0],
        section_down[0],
        backup_up.reshape(backup_up.shape[3:]),
        backup_down.reshape(backup_down.shape[3:]),
    )

    least = batch_count // 2
    stride = -(-(batch_count - least + 1) // 3)
    counts = list(range(batch_count, least - 1, -stride))
    chosen = (batch_count - live_count) // stride

    def variant(failed, count):
        return lambda *arrays: relay(*arrays, S, T, R, count, failed)

    variants = [variant(f, count) for count in counts for f in range(S)]
    return lax.switch(chosen * S + failed_section[0] % S, variants, *operands)


def solution(mesh):
    placed = (
        P("section", "dp", "tensor"),
        P("section", "dp", "tensor"),
        P("dp", "section", "tensor", None, None),
        P("dp", "section", "tensor", None, None),
        P("section", None),
        P(None, "dp", "tensor"),
        P(),
        P(),
    )
    return jax.shard_map(
        body, mesh=mesh, in_specs=placed, out_specs=P("section", "dp", "tensor"), check_vma=False
    )
```
